32 devices in a mesh: groups: 2 (over y), section: 4 (over z), seq: 4 (over x, core).
Axes of the slice: x: 2, y: 2, z: 4, core: 2. Of those that a mesh axis runs over, the one named last changes fastest.
Arguments:
- tokens: bfloat16 [8, 256, 1440], P('groups', 'seq'), parts along dimension 0, may hold values from -6 to 6
- block_order: int32 [8], P('groups'), parts along dimension 0, may hold values from 0 to 3, each once
- prompt_lengths: int32 [8], P('groups'), parts along dimension 0, may hold values from 1 to 256, 576 in all
- norm_gain: float32 [4, 1440], P('section'), may hold values from 0.1 to 1.9
- w_query: bfloat16 [4, 1440, 2048], P('section', None, 'seq'), may hold values from -4 to 4
- w_key_value: bfloat16 [4, 1440, 512], P('section'), may hold values from -4 to 4
- w_out: bfloat16 [4, 2048, 1440], P('section', 'seq'), may hold values from -0.125 to 0.125
- sink_logits: float32 [4, 32], P('section'), may hold values from 0 to 4
Outputs:
- hidden_states: bfloat16 [4, 8, 256, 1440], P('section', 'groups', 'seq'), parts along dimension 1
- layer_cache: bfloat16 [4, 8, 256, 512], P('section', 'groups', 'seq'), parts along dimension 1
The draws below stay inside these ranges and needn't reach their ends.
There are 2 independent parts, one for each index of `groups`. The reference program is written for one: setup_inputs(seed, part) draws one part's arguments, and reference() takes and returns one part's arrays. A program takes and returns all parts, laid end to end along the dimension named above; an argument that names none is the same for every part. Nothing has to cross between parts.
Inputs may be any that keep to these rules, and one draw needn't show every extreme that they name: `block_order`: each of 0 to 3 exactly once. `prompt_lengths`: the longest prompt is full.
All inputs are finite; a program needn't handle non-finite values.
Results may differ from the reference program's by a relative error of at most 0.024.
Values may be sent and summed in bfloat16 or wider, within the bound.
No kernel may reach another device: no remote copies, remote signals or barrier semaphores. Data moves between devices by JAX's collectives and lax.ppermute only.
A program may use at most 128 MiB of HBM per device.

```python
import math
import jax
import jax.numpy as jnp
import numpy as np
from jax import lax

D = 1440
HEADS = 32
KV_HEADS = 4
HEAD_DIM = 64
WIN = 128
MICRO = 4
BLOCK = 256
LAYERS = 4


def base_keys(key):
    drawn = jax.random.normal(jax.random.fold_in(key, 7), (LAYERS, D, 2 * KV_HEADS * HEAD_DIM), jnp.float32)
    return drawn * D ** (-0.5)


def draw_w_key_value(key, part):
    return jnp.clip(base_keys(key), -4.0, 4.0).astype(jnp.bfloat16)


def draw_w_query(key, part):
    drawn = jax.random.normal(jax.random.fold_in(key, 1), (LAYERS, D, HEADS * HEAD_DIM), jnp.float32) * D ** (-0.5)
    return jnp.clip(drawn, -4.0, 4.0).astype(jnp.bfloat16)


def steps_of(own_key, extent, cuts, least, top_value):
    def one(position, blocks):
        heights = jax.random.uniform(jax.random.fold_in(jax.random.fold_in(own_key, 6), position), (blocks,), jnp.float32, least / len(cuts), top_value / len(cuts))
        return jnp.repeat(jnp.exp(heights), extent[position] // blocks).reshape((-1,) + (1,) * (len(extent) - position - 1))

    loudness = one(*cuts[0])
    for cut in cuts[1:]:
        loudness = loudness * one(*cut)
    return loudness


def length_profile(count, total, limit, lean):
    loads = [(1 << 20) // math.isqrt(rank ** lean) + 1 for rank in range(2, count + 1)]
    surplus, holding = total - limit - (count - 1), [1] * (count - 1)
    while surplus > 0:
        free = [i for i in range(count - 1) if holding[i] < limit]
        whole, left = sum([loads[i] for i in free]), surplus
        for i in free:
            addition = min(limit - holding[i], max(1, left * loads[i] // whole), surplus)
            holding[i] = holding[i] + addition
            surplus = surplus - addition
    return np.array([limit] + holding)


def uneven_parts(key, amount, total, most, lean):
    if amount == 2:
        one = jax.random.randint(key, (), max(1, total - most), min(most, total - 1) + 1)
        return jnp.stack([one, total - one])
    tallies = jnp.asarray(length_profile(amount, total, most, lean), jnp.int32)
    couples = (amount - 1) // 2
    giver, receiver = tallies[1:1 + 2 * couples:2], tallies[2:2 + 2 * couples:2]
    margin = jnp.minimum(giver - 1, most - receiver)
    shifted = jax.random.randint(jax.random.fold_in(key, 1), (couples,), 0, 1 << 20) % (margin + 1)
    tallies = tallies.at[1:1 + 2 * couples:2].set(giver - shifted).at[2:2 + 2 * couples:2].set(receiver + shifted)
    return tallies[jax.random.permutation(jax.random.fold_in(key, 2), amount)]


def noise(rng, shape, spread, reach, pieces=(), kind=jnp.bfloat16):
    level = steps_of(rng, shape, pieces, -0.22, 0.18) if pieces else 1.0
    entries = jax.random.normal(rng, shape, jnp.float32) * spread * level
    return jnp.minimum(jnp.maximum(entries, -reach), reach).astype(kind)


def setup_inputs(seed: int = 0, part: int = 0) -> dict:
    arg_keys = jax.random.split(jax.random.key(seed), 9)
    part_keys = jax.random.split(jax.random.fold_in(arg_keys[8], part), 9)
    tokens = noise(part_keys[0], (MICRO, BLOCK, D), 1.0, 6.0, ((1, 4),))
    block_order = jax.random.permutation(part_keys[1], MICRO).astype(jnp.int32)
    prompt_lengths = uneven_parts(part_keys[2], MICRO, 9 * MICRO * BLOCK // 16, BLOCK, 2).astype(jnp.int32)
    norm_gain = jnp.clip(1.0 + 0.18 * jax.random.normal(arg_keys[3], (LAYERS, D), jnp.float32), 0.1, 1.9)
    w_query = draw_w_query(jax.random.fold_in(arg_keys[8], 71), part)
    w_key_value = draw_w_key_value(jax.random.fold_in(arg_keys[8], 71), part)
    w_out = noise(arg_keys[6], (LAYERS, HEADS * HEAD_DIM, D), (HEADS * HEAD_DIM) ** -0.5, 0.125, ((0, 4), (1, 4)))
    sink_logits = jnp.clip(4.0 * jax.random.uniform(arg_keys[7], (LAYERS, HEADS), jnp.float32) ** steps_of(arg_keys[7], (LAYERS, HEADS), ((0, 4),), -0.2, 0.2), 0.0, 4.0)
    return dict(tokens=tokens, block_order=block_order, prompt_lengths=prompt_lengths, norm_gain=norm_gain, w_query=w_query, w_key_value=w_key_value, w_out=w_out, sink_logits=sink_logits)


THETA = 150000.0
EPSILON = 1e-05

def rotary(positions, head_size):
    half = head_size // 2
    freq = jnp.exp(jnp.arange(half, dtype=jnp.float32) * (-2.0 * math.log(THETA) / head_size))
    angles = positions.astype(jnp.float32)[:, None] * freq[None, :]
    return (jnp.cos(angles)[:, None, :], jnp.sin(angles)[:, None, :])

def rotate(values, cosine, sine):
    half = values.shape[-1] // 2
    first = values[..., :half]
    second = values[..., half:]
    return jnp.concatenate([first * cosine - second * sine, second * cosine + first * sine], -1)

def layer_step(hidden, gain, w_query, w_key_value, w_out, sinks, cosine, sine, allowed):
    group = HEADS // KV_HEADS
    kv_width = KV_HEADS * HEAD_DIM
    count = hidden.shape[0]
    widened = hidden.astype(jnp.float32)
    scale = lax.rsqrt(lax.optimization_barrier(jnp.mean(widened * widened, -1, keepdims=True)) + EPSILON)
    normed = (widened * scale * gain).astype(jnp.bfloat16)
    queries = jnp.dot(normed, w_query, preferred_element_type=jnp.float32).reshape(count, HEADS, HEAD_DIM)
    queries = rotate(queries, cosine, sine).astype(jnp.bfloat16)
    projected = jnp.dot(normed, w_key_value, preferred_element_type=jnp.float32)
    keys = rotate(projected[:, :kv_width].reshape(count, KV_HEADS, HEAD_DIM), cosine, sine).reshape(count, kv_width)
    cache = jnp.concatenate([keys, projected[:, kv_width:]], 1).astype(jnp.bfloat16)
    key_heads = cache[:, :kv_width].reshape(count, KV_HEADS, HEAD_DIM).astype(jnp.float32)
    value_heads = cache[:, kv_width:].reshape(count, KV_HEADS, HEAD_DIM).astype(jnp.float32)
    grouped = queries.reshape(count, KV_HEADS, group, HEAD_DIM).astype(jnp.float32)
    scores = jnp.einsum('qkgd,skd->kgqs', grouped, key_heads) * 0.125
    sink = sinks.reshape(KV_HEADS, group)[:, :, None]
    masked = jnp.where(allowed, scores, jnp.float32(-1e+30))
    top = jnp.maximum(lax.optimization_barrier(jnp.max(masked, -1)), sink)
    expo = jnp.where(allowed, jnp.exp(scores - top[..., None]), jnp.float32(0.0))
    total = lax.optimization_barrier(jnp.sum(expo, -1)) + jnp.exp(sink - top)
    weights = (expo / total[..., None]).astype(jnp.bfloat16)
    context = jnp.einsum('kgqs,skd->qkgd', weights.astype(jnp.float32), value_heads)
    context = context.reshape(count, HEADS * HEAD_DIM).astype(jnp.bfloat16)
    output = jnp.dot(context, w_out, preferred_element_type=jnp.float32)
    return ((widened + output).astype(jnp.bfloat16), cache)

def reference(tokens, block_order, prompt_lengths, norm_gain, w_query, w_key_value, w_out, sink_logits):
    positions = jnp.arange(BLOCK, dtype=jnp.int32)
    cosine, sine = rotary(positions, HEAD_DIM)
    within = (positions[None, :] <= positions[:, None]) & (positions[:, None] - positions[None, :] < WIN)
    hidden_rows = [[] for layer in range(LAYERS)]
    cache_rows = [[] for layer in range(LAYERS)]
    for slot in range(MICRO):
        block = block_order[slot]
        hidden = lax.dynamic_index_in_dim(tokens, block, 0, keepdims=False)
        length = lax.dynamic_index_in_dim(prompt_lengths, block, 0, keepdims=False)
        allowed = within & ((positions[None, :] < length) | (positions[None, :] == positions[:, None]))
        for layer in range(LAYERS):
            hidden, cache = layer_step(hidden, norm_gain[layer], w_query[layer], w_key_value[layer], w_out[layer], sink_logits[layer], cosine, sine, allowed)
            hidden_rows[layer].append(hidden)
            cache_rows[layer].append(cache)
    hidden_states = jnp.stack([jnp.stack(row) for row in hidden_rows])
    layer_cache = jnp.stack([jnp.stack(row) for row in cache_rows])
    return (hidden_states, layer_cache)
```

```python
import functools
import math

import jax
import jax.numpy as jnp
from jax import lax
from jax.experimental import pallas as pl
from jax.experimental.pallas import tpu as pltpu
from jax.sharding import PartitionSpec as P

HEAD_DIM = 64
WIN = 128
THETA = 150000.0
EPSILON = 1e-05


VMEM = pl.BlockSpec(memory_space=pltpu.VMEM)
SMEM = pl.BlockSpec(memory_space=pltpu.SMEM)


def from_behind(block, axis, distance):
    devices = range(lax.axis_size(axis))
    route = [(i - distance, i) for i in devices if i - distance in devices]
    return lax.ppermute(block, axis, route)


def exchange(block, axis, mask):
    return lax.ppermute(block, axis, [(i, i ^ mask) for i in range(lax.axis_size(axis))])


def put(buffer, block, index, offset=0):
    zero = jnp.int32(0)
    return lax.dynamic_update_slice(buffer, block[None], (index, jnp.int32(offset), zero))


def gather_weight(shard):
    if lax.axis_size("seq") != 4 or lax.axis_size("groups") != 2 or shard.shape[0] % 32:
        return lax.all_gather(shard, "seq", axis=0)
    me = lax.axis_index("seq")
    group = lax.axis_index("groups")
    half = shard.shape[0] // 2
    mine = lax.dynamic_slice_in_dim(shard, group * half, half, 0)
    across = exchange(mine, "seq", 2)
    near = exchange(shard, "seq", 1)
    other = exchange(across, "groups", 1)
    far = jnp.zeros(shard.shape, shard.dtype)
    far = lax.dynamic_update_slice_in_dim(far, across, group * half, 0)
    far = lax.dynamic_update_slice_in_dim(far, other, (1 - group) * half, 0)
    diagonal = exchange(far, "seq", 1)
    whole = jnp.zeros((4,) + shard.shape, shard.dtype)
    whole = put(whole, shard, me)
    whole = put(whole, near, me ^ 1)
    whole = put(whole, far, me ^ 2)
    return put(whole, diagonal, me ^ 3)


def turned(values, cosine, sine):
    width = values.shape[-1]
    half = HEAD_DIM // 2
    lane = lax.broadcasted_iota(jnp.int32, values.shape, 1)
    ahead = pltpu.roll(values, width - half, 1)
    behind = pltpu.roll(values, half, 1)
    swapped = jnp.where((lane % HEAD_DIM) < half, ahead, behind)
    return values * cosine + swapped * sine


def key_kernel(kv_width, flag, arriving, entering, gain, pair, cosine, sine, hidden_out, normed_out, cache_out):
    hidden = jnp.where(flag[0] == 1, entering[...].astype(jnp.float32), arriving[...].astype(jnp.float32))
    hidden_out[...] = hidden.astype(jnp.bfloat16)
    scale = lax.rsqrt(jnp.mean(hidden * hidden, -1, keepdims=True) + EPSILON)
    normed = (hidden * scale * gain[...]).astype(jnp.bfloat16)
    normed_out[...] = normed
    projected = jnp.dot(normed, pair[...], preferred_element_type=jnp.float32)
    repeat = kv_width // cosine.shape[1]
    cos = jnp.concatenate([cosine[...]] * repeat, 1)
    sin = jnp.concatenate([sine[...]] * repeat, 1)
    keys = turned(projected[:, :kv_width], cos, sin)
    cache_out[:, :kv_width] = keys.astype(jnp.bfloat16)
    cache_out[:, kv_width:] = projected[:, kv_width:].astype(jnp.bfloat16)


def query_kernel(normed, weight, cosine, sine, queries_out):
    projected = jnp.dot(normed[...], weight[0], preferred_element_type=jnp.float32)
    repeat = projected.shape[1] // cosine.shape[1]
    cos = jnp.concatenate([cosine[...]] * repeat, 1)
    sin = jnp.concatenate([sine[...]] * repeat, 1)
    queries_out[...] = turned(projected, cos, sin).astype(jnp.bfloat16)


def attend_kernel(depth, kv_heads, scalars, sink, hidden, queries, *rest):
    pieces = rest[: depth + 1]
    out_weight, result, weight, semaphore = rest[depth + 1 :]
    copy = pltpu.make_async_copy(out_weight, weight, semaphore)
    copy.start()
    rows = hidden.shape[0]
    kv_width = kv_heads * HEAD_DIM
    span = rows * (depth + 1)
    heads = queries.shape[1] // HEAD_DIM
    pairs = heads // kv_heads // 2
    start, length = scalars[0], scalars[1]
    row = start + lax.broadcasted_iota(jnp.int32, (rows, span), 0)
    col = start - depth * rows + lax.broadcasted_iota(jnp.int32, (rows, span), 1)
    allowed = (col <= row) & (row - col < WIN) & (col >= 0) & ((col < length) | (col == row))
    bias = jnp.where(allowed, jnp.float32(0.0), jnp.float32(-1e30))
    bias = jnp.concatenate([bias] * pairs, 0)
    lane = lax.broadcasted_iota(jnp.int32, (span, 2 * HEAD_DIM), 1)
    low = lane < HEAD_DIM
    zero = jnp.float32(0.0)

    def halves(offset, index):
        base = offset + 2 * HEAD_DIM * (index // 2)
        slab = jnp.concatenate([p[:, base : base + 2 * HEAD_DIM] for p in pieces], 0)
        slab = slab.astype(jnp.float32)
        moved = pltpu.roll(slab, HEAD_DIM, 1)
        first, second = (slab, moved) if index % 2 == 0 else (moved, slab)
        return (
            jnp.where(low, first, zero).astype(jnp.bfloat16),
            jnp.where(low, zero, second).astype(jnp.bfloat16),
        )

    contexts = []
    for g in range(kv_heads):
        base = g * pairs * 2 * HEAD_DIM
        stacked = jnp.concatenate(
            [queries[:, base + p * 2 * HEAD_DIM : base + (p + 1) * 2 * HEAD_DIM] for p in range(pairs)], 0
        )
        context = None
        for side, (keys, values) in enumerate(zip(halves(0, g), halves(kv_width, g))):
            scores = lax.dot_general(
                stacked, keys, (((1,), (1,)), ((), ())), preferred_element_type=jnp.float32
            )
            masked = scores * 0.125 + bias
            limit = jnp.concatenate(
                [jnp.full((rows, 1), sink[(g * pairs + p) * 2 + side], jnp.float32) for p in range(pairs)], 0
            )
            top = jnp.maximum(jnp.max(masked, -1, keepdims=True), limit)
            expo = jnp.exp(masked - top)
            total = jnp.sum(expo, -1, keepdims=True) + jnp.exp(limit - top)
            weights = (expo * (1.0 / total)).astype(jnp.bfloat16)
            part = jnp.dot(weights, values, preferred_element_type=jnp.float32)
            context = part if context is None else context + part
        context = context.astype(jnp.bfloat16)
        contexts += [context[p * rows : (p + 1) * rows] for p in range(pairs)]
    joined = jnp.concatenate(contexts, 1)
    copy.wait()
    output = jnp.dot(joined, weight[...], preferred_element_type=jnp.float32)
    result[...] = (hidden[...].astype(jnp.float32) + output).astype(jnp.bfloat16)


def per_device(
    tokens, block_order, prompt_lengths, norm_gain, w_query, w_key_value, w_out, sink_logits
):
    section_index = lax.axis_index("section")
    sections = lax.axis_size("section")
    seq_index = lax.axis_index("seq")
    micro, rows, width = tokens.shape
    pair_weight = w_key_value[0]
    gain = norm_gain
    kv_width = pair_weight.shape[1] // 2
    kv_heads = kv_width // HEAD_DIM
    sink = sink_logits[0]
    depth = -(-WIN // rows)
    start = seq_index * rows
    half = HEAD_DIM // 2
    freq = jnp.exp(jnp.arange(half, dtype=jnp.float32) * (-2.0 * math.log(THETA) / HEAD_DIM))
    positions = start + jnp.arange(rows, dtype=jnp.int32)
    angles = positions.astype(jnp.float32)[:, None] * freq[None, :]
    cos, sin = jnp.cos(angles), jnp.sin(angles)
    cosine = jnp.concatenate([cos] * 4, 1)
    sine = jnp.concatenate([-sin, sin] * 2, 1)
    flag = (section_index == 0).astype(jnp.int32).reshape(1)
    entering = [
        lax.dynamic_index_in_dim(tokens, block_order[m], 0, keepdims=False) for m in range(micro)
    ]
    lengths = prompt_lengths[block_order]

    query_weight = gather_weight(w_query[0])
    out_weight = gather_weight(w_out[0])
    blocks, _, columns = query_weight.shape
    heads_width = blocks * columns
    out_weight = out_weight.reshape(heads_width, width)
    span = rows * (depth + 1)

    key_call = pl.pallas_call(
        functools.partial(key_kernel, kv_width),
        out_shape=(
            jax.ShapeDtypeStruct((rows, width), jnp.bfloat16),
            jax.ShapeDtypeStruct((rows, width), jnp.bfloat16),
            jax.ShapeDtypeStruct((rows, 2 * kv_width), jnp.bfloat16),
        ),
        in_specs=[SMEM] + [VMEM] * 6,
        out_specs=(VMEM, VMEM, VMEM),
        cost_estimate=pl.CostEstimate(
            flops=4 * rows * width * kv_width, bytes_accessed=2 * width * kv_width * 2, transcendentals=0
        ),
        name="keys",
    )
    query_call = pl.pallas_call(
        query_kernel,
        grid=(blocks,),
        out_shape=jax.ShapeDtypeStruct((rows, heads_width), jnp.bfloat16),
        in_specs=[
            pl.BlockSpec((rows, width), lambda j: (0, 0)),
            pl.BlockSpec((1, width, columns), lambda j: (j, 0, 0)),
            pl.BlockSpec((rows, 2 * HEAD_DIM), lambda j: (0, 0)),
            pl.BlockSpec((rows, 2 * HEAD_DIM), lambda j: (0, 0)),
        ],
        out_specs=pl.BlockSpec((rows, columns), lambda j: (0, j)),
        cost_estimate=pl.CostEstimate(
            flops=2 * rows * width * heads_width, bytes_accessed=2 * width * heads_width, transcendentals=0
        ),
        name="queries",
    )
    attend_call = pl.pallas_call(
        functools.partial(attend_kernel, depth, kv_heads),
        out_shape=jax.ShapeDtypeStruct((rows, width), jnp.bfloat16),
        in_specs=[SMEM, SMEM] + [VMEM] * (3 + depth) + [pl.BlockSpec(memory_space=pl.ANY)],
        out_specs=VMEM,
        scratch_shapes=[pltpu.VMEM((heads_width, width), jnp.bfloat16), pltpu.SemaphoreType.DMA],
        cost_estimate=pl.CostEstimate(
            flops=2 * rows * width * heads_width + 4 * rows * span * heads_width,
            bytes_accessed=2 * width * heads_width,
            transcendentals=rows * span * heads_width // HEAD_DIM,
        ),
        name="attend",
    )

    arriving = jnp.zeros((rows, width), jnp.bfloat16)
    hiddens, caches = [], []
    turns = micro + sections - 1
    for counter in range(turns):
        slot = jnp.clip(counter - section_index, 0, micro - 1)
        scalars = jnp.stack([start, lengths[slot]])
        hidden, normed, cache = key_call(
            flag, arriving, entering[min(counter, micro - 1)], gain, pair_weight, cosine, sine
        )
        window = [from_behind(cache, "seq", offset) for offset in range(depth, 0, -1)]
        queries = query_call(normed, query_weight, cosine, sine)
        updated = attend_call(scalars, sink, hidden, queries, *window, cache, out_weight)
        hiddens.append(updated)
        caches.append(cache)
        if counter < turns - 1:
            arriving = from_behind(updated, "section", 1)
    hidden_states = lax.dynamic_slice_in_dim(jnp.stack(hiddens), section_index, micro, 0)
    layer_cache = lax.dynamic_slice_in_dim(jnp.stack(caches), section_index, micro, 0)
    return (hidden_states[None], layer_cache[None])


def solution(mesh):
    in_specs = (
        P("groups", "seq", None),
        P("groups"),
        P("groups"),
        P("section", None),
        P("section", None, "seq"),
        P("section", None, None),
        P("section", "seq", None),
        P("section", None),
    )
    out_specs = (P("section", "groups", "seq", None), P("section", "groups", "seq", None))
    return jax.shard_map(
        per_device, mesh=mesh, in_specs=in_specs, out_specs=out_specs, check_vma=False
    )
```

```python
import functools
import math

import jax
import jax.numpy as jnp
from jax import lax
from jax.experimental import pallas as pl
from jax.experimental.pallas import tpu as pltpu
from jax.sharding import PartitionSpec as P

HEAD_DIM = 64
WIN = 128
THETA = 150000.0
EPSILON = 1e-05


VMEM = pl.BlockSpec(memory_space=pltpu.VMEM)
SMEM = pl.BlockSpec(memory_space=pltpu.SMEM)


def from_behind(block, axis, distance):
    devices = range(lax.axis_size(axis))
    route = [(i - distance, i) for i in devices if i - distance in devices]
    return lax.ppermute(block, axis, route)


def exchange(block, axis, mask):
    return lax.ppermute(block, axis, [(i, i ^ mask) for i in range(lax.axis_size(axis))])


def swapped_gather():
    return lax.axis_size("seq") == 4 and lax.axis_size("groups") == 2


def gather_weight(shard, mine):
    if mine is None:
        whole = lax.all_gather(shard, "seq", axis=0)
        return [whole], [(0, j, j, None) for j in range(whole.shape[0])], None
    across = exchange(mine, "seq", 2)

    def rest(across):
        near = exchange(shard, "seq", 1)
        other = exchange(across, "groups", 1)
        parts = [shard, near, across, exchange(across, "seq", 1), other, exchange(other, "seq", 1)]
        plan = [(0, 0), (1, 1), (2, 2), (3, 3), (4, 2), (5, 3)]
        return [p[None] for p in parts], [
            (i, 0, block, None if i < 2 else ("mine" if i < 4 else "other")) for i, block in plan
        ]

    return across, rest


def turned(values, cosine, sine):
    width = values.shape[-1]
    half = HEAD_DIM // 2
    lane = lax.broadcasted_iota(jnp.int32, values.shape, 1)
    ahead = pltpu.roll(values, width - half, 1)
    behind = pltpu.roll(values, half, 1)
    swapped = jnp.where((lane % HEAD_DIM) < half, ahead, behind)
    return values * cosine + swapped * sine


def key_kernel(kv_width, flag, arriving, entering, gain, pair, cosine, sine, hidden_out, normed_out, cache_out):
    hidden = jnp.where(flag[1] == 0, entering[...].astype(jnp.float32), arriving[...].astype(jnp.float32))
    hidden_out[...] = hidden.astype(jnp.bfloat16)
    scale = lax.rsqrt(jnp.mean(hidden * hidden, -1, keepdims=True) + EPSILON)
    normed = (hidden * scale * gain[...]).astype(jnp.bfloat16)
    normed_out[...] = normed
    projected = jnp.dot(normed, pair[...], preferred_element_type=jnp.float32)
    repeat = kv_width // cosine.shape[1]
    times = hidden.shape[0] // cosine.shape[0]
    cos = jnp.concatenate([jnp.concatenate([cosine[...]] * repeat, 1)] * times, 0)
    sin = jnp.concatenate([jnp.concatenate([sine[...]] * repeat, 1)] * times, 0)
    keys = turned(projected[:, :kv_width], cos, sin)
    cache_out[:, :kv_width] = keys.astype(jnp.bfloat16)
    cache_out[:, kv_width:] = projected[:, kv_width:].astype(jnp.bfloat16)


def fetches(plan, info, parts, weight, semaphores):
    height = weight.shape[1]
    half = height // 2
    copies = []
    for number, (part, entry, block, side) in enumerate(plan):
        target = weight.at[block]
        if side is not None:
            group = info[2] if side == "mine" else 1 - info[2]
            target = weight.at[block, pl.ds(pl.multiple_of(group * half, 16), half)]
        copies.append(pltpu.make_async_copy(parts[part].at[entry], target, semaphores.at[number]))
    for copy in copies:
        copy.start()
    return copies


def query_kernel(plan, info, normed, cosine, sine, *rest):
    parts, (queries_out, weight, semaphores) = rest[:-3], rest[-3:]
    copies = fetches(plan, info, parts, weight, semaphores)
    blocks, _, columns = weight.shape
    times = normed.shape[0] // cosine.shape[0]
    repeat = columns // cosine.shape[1]
    cos = jnp.concatenate([jnp.concatenate([cosine[...]] * repeat, 1)] * times, 0)
    sin = jnp.concatenate([jnp.concatenate([sine[...]] * repeat, 1)] * times, 0)
    for j in range(blocks):
        for copy, (_, _, block, _) in zip(copies, plan):
            if block == j:
                copy.wait()
        projected = jnp.dot(normed[...], weight[j], preferred_element_type=jnp.float32)
        queries_out[:, j * columns : (j + 1) * columns] = turned(projected, cos, sin).astype(jnp.bfloat16)


def attend_kernel(shape, plan, info, sink, hidden, queries, *rest):
    depth, kv_heads, rows, fast, counter, chunks = shape
    pieces = rest[: depth + 1]
    parts, (result, weight, contexts, semaphores) = rest[depth + 1 : -4], rest[-4:]
    copies = fetches(plan, info, parts, weight, semaphores)
    times = hidden.shape[0] // rows
    blocks, _, columns = weight.shape
    kv_width = kv_heads * HEAD_DIM
    span = rows * (depth + 1)
    wide = 2 * HEAD_DIM
    pairs = columns // wide
    group = blocks * columns // HEAD_DIM // kv_heads
    start = info[0]
    chunk = jnp.clip(counter - info[1], 0, chunks - 1)
    row = start + lax.broadcasted_iota(jnp.int32, (rows, span), 0)
    col = start - depth * rows + lax.broadcasted_iota(jnp.int32, (rows, span), 1)
    within = (col <= row) & (row - col < WIN) & (col >= 0)
    lane = lax.broadcasted_iota(jnp.int32, (span, wide), 1)
    low = lane < HEAD_DIM
    zero = jnp.float32(0.0)

    def one(step, carry):
        prompt, block = step // blocks, step % blocks
        above = pl.multiple_of(prompt * rows, rows)
        left = pl.multiple_of(block * columns, columns)
        length = info[4 + chunk * times + prompt]
        allowed = within & ((col < length) | (col == row))
        bias = jnp.where(allowed, zero, jnp.float32(-1e30))
        bias = jnp.concatenate([bias] * pairs, 0)
        first_head = (info[3] ^ block if fast else block) * (2 * pairs)
        index = first_head // group
        even = index % 2 == 0

        def halves(offset):
            base = pl.multiple_of(offset + wide * (index // 2), wide)
            slab = jnp.concatenate([p[pl.ds(above, rows), pl.ds(base, wide)] for p in pieces], 0)
            slab = slab.astype(jnp.float32)
            moved = pltpu.roll(slab, HEAD_DIM, 1)
            first, second = jnp.where(even, slab, moved), jnp.where(even, moved, slab)
            return (
                jnp.where(low, first, zero).astype(jnp.bfloat16),
                jnp.where(low, zero, second).astype(jnp.bfloat16),
            )

        band = queries[pl.ds(above, rows), pl.ds(left, columns)]
        stacked = jnp.concatenate([band[:, p * wide : (p + 1) * wide] for p in range(pairs)], 0)
        context = None
        for side, (keys, values) in enumerate(zip(halves(0), halves(kv_width))):
            scores = lax.dot_general(
                stacked, keys, (((1,), (1,)), ((), ())), preferred_element_type=jnp.float32
            )
            masked = scores * 0.125 + bias
            limit = jnp.concatenate(
                [jnp.full((rows, 1), sink[first_head + 2 * p + side], jnp.float32) for p in range(pairs)], 0
            )
            top = jnp.maximum(jnp.max(masked, -1, keepdims=True), limit)
            expo = jnp.exp(masked - top)
            total = jnp.sum(expo, -1, keepdims=True) + jnp.exp(limit - top)
            weights = (expo * (1.0 / total)).astype(jnp.bfloat16)
            part = jnp.dot(weights, values, preferred_element_type=jnp.float32)
            context = part if context is None else context + part
        context = context.astype(jnp.bfloat16)
        joined = jnp.concatenate([context[p * rows : (p + 1) * rows] for p in range(pairs)], 1)
        contexts[pl.ds(above, rows), pl.ds(left, columns)] = joined
        return carry

    lax.fori_loop(0, times * blocks, one, 0, unroll=2)
    for copy in copies:
        copy.wait()
    output = hidden[...].astype(jnp.float32)
    for block in range(blocks):
        output = output + lax.dot_general(
            contexts[:, block * columns : (block + 1) * columns],
            weight[block],
            (((1,), (1,)), ((), ())),
            preferred_element_type=jnp.float32,
        )
    result[...] = output.astype(jnp.bfloat16)


def per_device(
    tokens, block_order, prompt_lengths, norm_gain, w_query, w_key_value, w_out, sink_logits
):
    section_index = lax.axis_index("section")
    sections = lax.axis_size("section")
    seq_index = lax.axis_index("seq")
    micro, rows, width = tokens.shape
    pair_weight = w_key_value[0]
    gain = norm_gain
    kv_width = pair_weight.shape[1] // 2
    kv_heads = kv_width // HEAD_DIM
    sink = sink_logits[0]
    depth = -(-WIN // rows)
    start = seq_index * rows
    half = HEAD_DIM // 2
    freq = jnp.exp(jnp.arange(half, dtype=jnp.float32) * (-2.0 * math.log(THETA) / HEAD_DIM))
    positions = start + jnp.arange(rows, dtype=jnp.int32)
    angles = positions.astype(jnp.float32)[:, None] * freq[None, :]
    cos, sin = jnp.cos(angles), jnp.sin(angles)
    cosine = jnp.concatenate([cos] * 4, 1)
    sine = jnp.concatenate([-sin, sin] * 2, 1)
    times = 2 if micro % 2 == 0 else 1
    chunks = micro // times
    tall = times * rows
    fast = swapped_gather()
    group_index = lax.axis_index("groups")
    lengths = prompt_lengths[block_order]
    head = jnp.stack([start, section_index, group_index, seq_index]).astype(jnp.int32)
    info = jnp.concatenate([head, lengths])
    entering = tokens[block_order].reshape(chunks, tall, width)

    turned_out = jnp.swapaxes(w_out[0], 0, 1)
    if fast:
        halved = [
            lax.dynamic_slice_in_dim(w, group_index * (w.shape[0] // 2), w.shape[0] // 2, 0)
            for w in (w_query[0], turned_out)
        ]
        across, rest = gather_weight(w_query[0], halved[0])
        across, entering, mine = lax.optimization_barrier((across, entering, halved[1]))
        query_parts, query_plan = rest(across)
        across, rest = gather_weight(turned_out, mine)
        out_parts, out_plan = rest(across)
    else:
        query_parts, query_plan, _ = gather_weight(w_query[0], None)
        out_parts, out_plan, _ = gather_weight(turned_out, None)
    blocks, columns = lax.axis_size("seq"), w_query.shape[2]
    heads_width = blocks * columns
    span = rows * (depth + 1)
    any_space = pl.BlockSpec(memory_space=pl.ANY)

    key_call = pl.pallas_call(
        functools.partial(key_kernel, kv_width),
        out_shape=(
            jax.ShapeDtypeStruct((tall, width), jnp.bfloat16),
            jax.ShapeDtypeStruct((tall, width), jnp.bfloat16),
            jax.ShapeDtypeStruct((tall, 2 * kv_width), jnp.bfloat16),
        ),
        in_specs=[SMEM] + [VMEM] * 6,
        out_specs=(VMEM, VMEM, VMEM),
        cost_estimate=pl.CostEstimate(
            flops=4 * tall * width * kv_width, bytes_accessed=2 * width * kv_width * 2, transcendentals=0
        ),
        name="keys",
    )
    query_call = pl.pallas_call(
        functools.partial(query_kernel, query_plan),
        out_shape=jax.ShapeDtypeStruct((tall, heads_width), jnp.bfloat16),
        in_specs=[SMEM] + [VMEM] * 3 + [any_space] * len(query_parts),
        out_specs=VMEM,
        scratch_shapes=[
            pltpu.VMEM((blocks, width, columns), jnp.bfloat16),
            pltpu.SemaphoreType.DMA((len(query_plan),)),
        ],
        cost_estimate=pl.CostEstimate(
            flops=2 * tall * width * heads_width, bytes_accessed=2 * width * heads_width, transcendentals=0
        ),
        name="queries",
    )

    def attend_call(counter):
        return pl.pallas_call(
            functools.partial(
                attend_kernel, (depth, kv_heads, rows, fast, counter, chunks), out_plan
            ),
            out_shape=jax.ShapeDtypeStruct((tall, width), jnp.bfloat16),
            in_specs=[SMEM, SMEM] + [VMEM] * (3 + depth) + [any_space] * len(out_parts),
            out_specs=VMEM,
            scratch_shapes=[
                pltpu.VMEM((blocks, width, columns), jnp.bfloat16),
                pltpu.VMEM((tall, heads_width), jnp.bfloat16),
                pltpu.SemaphoreType.DMA((len(out_plan),)),
            ],
            cost_estimate=pl.CostEstimate(
                flops=2 * tall * width * heads_width + 4 * tall * span * heads_width,
                bytes_accessed=2 * width * heads_width,
                transcendentals=tall * span * heads_width // HEAD_DIM,
            ),
            name="attend",
        )

    arriving = jnp.zeros((tall, width), jnp.bfloat16)
    hiddens, caches = [], []
    turns = chunks + sections - 1
    for counter in range(turns):
        hidden, normed, cache = key_call(
            info, arriving, entering[min(counter, chunks - 1)], gain, pair_weight, cosine, sine
        )
        window = [from_behind(cache, "seq", offset) for offset in range(depth, 0, -1)]
        queries = query_call(info, normed, cosine, sine, *query_parts)
        updated = attend_call(counter)(info, sink, hidden, queries, *window, cache, *out_parts)
        hiddens.append(updated)
        caches.append(cache)
        if counter < turns - 1:
            arriving = from_behind(updated, "section", 1)
    hidden_states = lax.dynamic_slice_in_dim(jnp.stack(hiddens), section_index, chunks, 0)
    layer_cache = lax.dynamic_slice_in_dim(jnp.stack(caches), section_index, chunks, 0)
    return (
        hidden_states.reshape(1, micro, rows, width),
        layer_cache.reshape(1, micro, rows, 2 * kv_width),
    )


def solution(mesh):
    in_specs = (
        P("groups", "seq", None),
        P("groups"),
        P("groups"),
        P("section", None),
        P("section", None, "seq"),
        P("section", None, None),
        P("section", "seq", None),
        P("section", None),
    )
    out_specs = (P("section", "groups", "seq", None), P("section", "groups", "seq", None))
    return jax.shard_map(
        per_device, mesh=mesh, in_specs=in_specs, out_specs=out_specs, check_vma=False
    )
```

```python
import functools
import math

import jax
import jax.numpy as jnp
from jax import lax
from jax.experimental import pallas as pl
from jax.experimental.pallas import tpu as pltpu
from jax.sharding import PartitionSpec as P

HEAD_DIM = 64
WIN = 128
THETA = 150000.0
EPSILON = 1e-05


VMEM = pl.BlockSpec(memory_space=pltpu.VMEM)
SMEM = pl.BlockSpec(memory_space=pltpu.SMEM)


def from_behind(block, axis, distance):
    devices = range(lax.axis_size(axis))
    route = [(i - distance, i) for i in devices if i - distance in devices]
    return lax.ppermute(block, axis, route)


def exchange(block, axis, mask):
    return lax.ppermute(block, axis, [(i, i ^ mask) for i in range(lax.axis_size(axis))])


def swapped_gather():
    return lax.axis_size("seq") == 4 and lax.axis_size("groups") == 2


def gather_weight(shard, mine):
    if mine is None:
        whole = lax.all_gather(shard, "seq", axis=0)
        return [whole], [(0, j, j, None) for j in range(whole.shape[0])], None
    across = exchange(mine, "seq", 2)

    def rest(across):
        near = exchange(shard, "seq", 1)
        other = exchange(across, "groups", 1)
        parts = [shard, near, across, exchange(across, "seq", 1), other, exchange(other, "seq", 1)]
        plan = [(0, 0), (1, 1), (2, 2), (3, 3), (4, 2), (5, 3)]
        return [p[None] for p in parts], [
            (i, 0, block, None if i < 2 else ("mine" if i < 4 else "other")) for i, block in plan
        ]

    return across, rest


def turned(values, cosine, sine):
    width = values.shape[-1]
    half = HEAD_DIM // 2
    lane = lax.broadcasted_iota(jnp.int32, values.shape, 1)
    ahead = pltpu.roll(values, width - half, 1)
    behind = pltpu.roll(values, half, 1)
    swapped = jnp.where((lane % HEAD_DIM) < half, ahead, behind)
    return values * cosine + swapped * sine


def key_kernel(kv_width, flag, arriving, entering, gain, pair, cosine, sine, hidden_out, normed_out, cache_out):
    hidden = jnp.where(flag[1] == 0, entering[...].astype(jnp.float32), arriving[...].astype(jnp.float32))
    hidden_out[...] = hidden.astype(jnp.bfloat16)
    scale = lax.rsqrt(jnp.mean(hidden * hidden, -1, keepdims=True) + EPSILON)
    normed = (hidden * scale * gain[...]).astype(jnp.bfloat16)
    normed_out[...] = normed
    projected = jnp.dot(normed, pair[...], preferred_element_type=jnp.float32)
    repeat = kv_width // cosine.shape[1]
    times = hidden.shape[0] // cosine.shape[0]
    cos = jnp.concatenate([jnp.concatenate([cosine[...]] * repeat, 1)] * times, 0)
    sin = jnp.concatenate([jnp.concatenate([sine[...]] * repeat, 1)] * times, 0)
    keys = turned(projected[:, :kv_width], cos, sin)
    cache_out[:, :kv_width] = keys.astype(jnp.bfloat16)
    cache_out[:, kv_width:] = projected[:, kv_width:].astype(jnp.bfloat16)


def fetches(plan, info, parts, weight, semaphores):
    height = weight.shape[1]
    half = height // 2
    copies = []
    for number, (part, entry, block, side) in enumerate(plan):
        target = weight.at[block]
        if side is not None:
            group = info[2] if side == "mine" else 1 - info[2]
            target = weight.at[block, pl.ds(pl.multiple_of(group * half, 16), half)]
        copies.append(pltpu.make_async_copy(parts[part].at[entry], target, semaphores.at[number]))
    for copy in copies:
        copy.start()
    return copies


def query_kernel(plan, info, normed, cosine, sine, *rest):
    parts, (queries_out, weight, semaphores) = rest[:-3], rest[-3:]
    copies = fetches(plan, info, parts, weight, semaphores)
    blocks, _, columns = weight.shape
    times = normed.shape[0] // cosine.shape[0]
    repeat = columns // cosine.shape[1]
    cos = jnp.concatenate([jnp.concatenate([cosine[...] * 0.125] * repeat, 1)] * times, 0)
    sin = jnp.concatenate([jnp.concatenate([sine[...] * 0.125] * repeat, 1)] * times, 0)
    for j in range(blocks):
        for copy, (_, _, block, _) in zip(copies, plan):
            if block == j:
                copy.wait()
        projected = jnp.dot(normed[...], weight[j], preferred_element_type=jnp.float32)
        queries_out[:, j * columns : (j + 1) * columns] = turned(projected, cos, sin).astype(jnp.bfloat16)


def attend_kernel(shape, plan, info, sink, hidden, queries, *rest):
    depth, kv_heads, rows, fast, counter, chunks = shape
    pieces = rest[: depth + 1]
    parts, (result, weight, contexts, semaphores) = rest[depth + 1 : -4], rest[-4:]
    copies = fetches(plan, info, parts, weight, semaphores)
    times = hidden.shape[0] // rows
    blocks, _, columns = weight.shape
    kv_width = kv_heads * HEAD_DIM
    span = rows * (depth + 1)
    wide = 2 * HEAD_DIM
    pairs = columns // wide
    group = blocks * columns // HEAD_DIM // kv_heads
    start = info[0]
    chunk = jnp.clip(counter - info[1], 0, chunks - 1)
    row = start + lax.broadcasted_iota(jnp.int32, (rows, span), 0)
    col = start - depth * rows + lax.broadcasted_iota(jnp.int32, (rows, span), 1)
    within = (col <= row) & (row - col < WIN) & (col >= 0)
    lane = lax.broadcasted_iota(jnp.int32, (span, wide), 1)
    low = lane < HEAD_DIM
    zero = jnp.float32(0.0)

    def one(step, carry):
        prompt, block = step // blocks, step % blocks
        above = pl.multiple_of(prompt * rows, rows)
        left = pl.multiple_of(block * columns, columns)
        length = info[4 + chunk * times + prompt]
        allowed = within & ((col < length) | (col == row))
        bias = jnp.where(allowed, zero, jnp.float32(-1e30))
        bias = jnp.concatenate([bias] * pairs, 0)
        first_head = (info[3] ^ block if fast else block) * (2 * pairs)
        index = first_head // group
        even = index % 2 == 0

        def halves(offset, filler):
            base = pl.multiple_of(offset + wide * (index // 2), wide)
            slab = jnp.concatenate([p[pl.ds(above, rows), pl.ds(base, wide)] for p in pieces], 0)
            slab = slab.astype(jnp.float32)
            moved = pltpu.roll(slab, HEAD_DIM, 1)
            first, second = jnp.where(even, slab, moved), jnp.where(even, moved, slab)
            return (
                jnp.where(low, first, filler).astype(jnp.bfloat16),
                jnp.where(low, filler, second).astype(jnp.bfloat16),
            )

        band = queries[pl.ds(above, rows), pl.ds(left, columns)]
        stacked = jnp.concatenate([band[:, p * wide : (p + 1) * wide] for p in range(pairs)], 0)
        sums, rests = [], []
        for side, (keys, values) in enumerate(zip(halves(0, zero), halves(kv_width, zero + 1.0))):
            scores = lax.dot_general(
                stacked, keys, (((1,), (1,)), ((), ())), preferred_element_type=jnp.float32
            )
            masked = scores + bias
            limit = jnp.concatenate(
                [jnp.full((rows, 1), sink[first_head + 2 * p + side], jnp.float32) for p in range(pairs)], 0
            )
            top = jnp.maximum(jnp.max(masked, -1, keepdims=True), limit)
            expo = jnp.exp(masked - top)
            rests.append(jnp.exp(limit - top))
            sums.append(jnp.dot(expo.astype(jnp.bfloat16), values, preferred_element_type=jnp.float32))
        left_half = lax.broadcasted_iota(jnp.int32, sums[0].shape, 1) < HEAD_DIM
        total = pltpu.roll(jnp.where(left_half, sums[1], sums[0]), HEAD_DIM, 1)
        total = total + jnp.where(left_half, rests[0], rests[1])
        context = (jnp.where(left_half, sums[0], sums[1]) / total).astype(jnp.bfloat16)
        joined = jnp.concatenate([context[p * rows : (p + 1) * rows] for p in range(pairs)], 1)
        contexts[pl.ds(above, rows), pl.ds(left, columns)] = joined
        return carry

    lax.fori_loop(0, times * blocks, one, 0, unroll=4)
    for copy in copies:
        copy.wait()
    output = hidden[...].astype(jnp.float32)
    for block in range(blocks):
        output = output + lax.dot_general(
            contexts[:, block * columns : (block + 1) * columns],
            weight[block],
            (((1,), (1,)), ((), ())),
            preferred_element_type=jnp.float32,
        )
    result[...] = output.astype(jnp.bfloat16)


def per_device(
    tokens, block_order, prompt_lengths, norm_gain, w_query, w_key_value, w_out, sink_logits
):
    section_index = lax.axis_index("section")
    sections = lax.axis_size("section")
    seq_index = lax.axis_index("seq")
    micro, rows, width = tokens.shape
    pair_weight = w_key_value[0]
    gain = norm_gain
    kv_width = pair_weight.shape[1] // 2
    kv_heads = kv_width // HEAD_DIM
    sink = sink_logits[0]
    depth = -(-WIN // rows)
    start = seq_index * rows
    half = HEAD_DIM // 2
    freq = jnp.exp(jnp.arange(half, dtype=jnp.float32) * (-2.0 * math.log(THETA) / HEAD_DIM))
    positions = start + jnp.arange(rows, dtype=jnp.int32)
    angles = positions.astype(jnp.float32)[:, None] * freq[None, :]
    cos, sin = jnp.cos(angles), jnp.sin(angles)
    cosine = jnp.concatenate([cos] * 4, 1)
    sine = jnp.concatenate([-sin, sin] * 2, 1)
    times = 2 if micro % 2 == 0 else 1
    chunks = micro // times
    tall = times * rows
    fast = swapped_gather()
    group_index = lax.axis_index("groups")
    lengths = prompt_lengths[block_order]
    head = jnp.stack([start, section_index, group_index, seq_index]).astype(jnp.int32)
    info = jnp.concatenate([head, lengths])
    entering = tokens[block_order].reshape(chunks, tall, width)

    turned_out = jnp.swapaxes(w_out[0], 0, 1)
    if fast:
        halved = [
            lax.dynamic_slice_in_dim(w, group_index * (w.shape[0] // 2), w.shape[0] // 2, 0)
            for w in (w_query[0], turned_out)
        ]
        across, rest = gather_weight(w_query[0], halved[0])
        across, entering, mine = lax.optimization_barrier((across, entering, halved[1]))
        query_parts, query_plan = rest(across)
        across_out = exchange(mine, "seq", 2)
    else:
        query_parts, query_plan, _ = gather_weight(w_query[0], None)
        out_parts, out_plan, _ = gather_weight(turned_out, None)
    blocks, columns = lax.axis_size("seq"), w_query.shape[2]
    heads_width = blocks * columns
    span = rows * (depth + 1)
    out_count = 6 if fast else len(out_parts)
    if fast:
        out_plan = query_plan
    any_space = pl.BlockSpec(memory_space=pl.ANY)

    key_call = pl.pallas_call(
        functools.partial(key_kernel, kv_width),
        out_shape=(
            jax.ShapeDtypeStruct((tall, width), jnp.bfloat16),
            jax.ShapeDtypeStruct((tall, width), jnp.bfloat16),
            jax.ShapeDtypeStruct((tall, 2 * kv_width), jnp.bfloat16),
        ),
        in_specs=[SMEM] + [VMEM] * 6,
        out_specs=(VMEM, VMEM, VMEM),
        cost_estimate=pl.CostEstimate(
            flops=4 * tall * width * kv_width, bytes_accessed=2 * width * kv_width * 2, transcendentals=0
        ),
        name="keys",
    )
    query_call = pl.pallas_call(
        functools.partial(query_kernel, query_plan),
        out_shape=jax.ShapeDtypeStruct((tall, heads_width), jnp.bfloat16),
        in_specs=[SMEM] + [VMEM] * 3 + [any_space] * len(query_parts),
        out_specs=VMEM,
        scratch_shapes=[
            pltpu.VMEM((blocks, width, columns), jnp.bfloat16),
            pltpu.SemaphoreType.DMA((len(query_plan),)),
        ],
        cost_estimate=pl.CostEstimate(
            flops=2 * tall * width * heads_width, bytes_accessed=2 * width * heads_width, transcendentals=0
        ),
        name="queries",
    )

    def attend_call(counter):
        return pl.pallas_call(
            functools.partial(
                attend_kernel, (depth, kv_heads, rows, fast, counter, chunks), out_plan
            ),
            out_shape=jax.ShapeDtypeStruct((tall, width), jnp.bfloat16),
            in_specs=[SMEM, SMEM] + [VMEM] * (3 + depth) + [any_space] * out_count,
            out_specs=VMEM,
            scratch_shapes=[
                pltpu.VMEM((blocks, width, columns), jnp.bfloat16),
                pltpu.VMEM((tall, heads_width), jnp.bfloat16),
                pltpu.SemaphoreType.DMA((len(out_plan),)),
            ],
            cost_estimate=pl.CostEstimate(
                flops=2 * tall * width * heads_width + 4 * tall * span * heads_width,
                bytes_accessed=2 * width * heads_width,
                transcendentals=tall * span * heads_width // HEAD_DIM,
            ),
            name="attend",
        )

    arriving = jnp.zeros((tall, width), jnp.bfloat16)
    hiddens, caches = [], []
    turns = chunks + sections - 1
    for counter in range(turns):
        hidden, normed, cache = key_call(
            info, arriving, entering[min(counter, chunks - 1)], gain, pair_weight, cosine, sine
        )
        if fast and counter == 0:
            across_out, normed = lax.optimization_barrier((across_out, normed))
            near_out = exchange(turned_out, "seq", 1)
            other_out = exchange(across_out, "groups", 1)
        window = [from_behind(cache, "seq", offset) for offset in range(depth, 0, -1)]
        queries = query_call(info, normed, cosine, sine, *query_parts)
        if fast and counter == 0:
            other_out, across_out, queries, *window = lax.optimization_barrier(
                (other_out, across_out, queries, *window)
            )
            passed = (exchange(across_out, "seq", 1), exchange(other_out, "seq", 1))
            out_parts = (turned_out, near_out, across_out, passed[0], other_out, passed[1])
            out_parts = [part[None] for part in out_parts]
        updated = attend_call(counter)(info, sink, hidden, queries, *window, cache, *out_parts)
        later, held = updated, cache
        if counter < turns - 1:
            later, held = lax.optimization_barrier((updated, cache))
        hiddens.append(later)
        caches.append(held)
        if counter < turns - 1:
            arriving = from_behind(updated, "section", 1)
    hidden_states = lax.dynamic_slice_in_dim(jnp.stack(hiddens), section_index, chunks, 0)
    layer_cache = lax.dynamic_slice_in_dim(jnp.stack(caches), section_index, chunks, 0)
    return (
        hidden_states.reshape(1, micro, rows, width),
        layer_cache.reshape(1, micro, rows, 2 * kv_width),
    )


def solution(mesh):
    in_specs = (
        P("groups", "seq", None),
        P("groups"),
        P("groups"),
        P("section", None),
        P("section", None, "seq"),
        P("section", None, None),
        P("section", "seq", None),
        P("section", None),
    )
    out_specs = (P("section", "groups", "seq", None), P("section", "groups", "seq", None))
    return jax.shard_map(
        per_device, mesh=mesh, in_specs=in_specs, out_specs=out_specs, check_vma=False
    )
```
